32 devices in a mesh: slab: 8 (over y, x, core), det: 4 (over z).
Axes of the slice: x: 2, y: 2, z: 4, core: 2. Of those that a mesh axis runs over, the one named last changes fastest.
Arguments:
- traces: float32 [32, 128, 4096], P(('slab', 'det')), may hold values from -6 to 6
- tables: bfloat16 [32, 256, 2048], P('slab', None, 'det'), may hold values from -0.0625 to 0.0625
- slab_range: int32 [32, 2], P(('slab', 'det')), may hold values from 0 to 7, as said below
- table_slot: int32 [32, 7], P(('slab', 'det')), may hold values from 0 to 3
- sample_start: int32 [32, 7], P(('slab', 'det')), may hold values from 0 to 3840
Outputs:
- image: float32 [128, 16384], P(None, ('slab', 'det'))
The draws below stay inside these ranges and needn't reach their ends.
Inputs may be any that keep to these rules, and one draw needn't show every extreme that they name: For detector d with home slab g = d // 4: max(0, g - 3) <= slab_range[d, 0] <= g <= slab_range[d, 1] <= min(7, g + 3); some detectors reach the full 3 on both sides where the grid allows.
All inputs are finite; a program needn't handle non-finite values.
Results may differ from the reference program's by a relative error of at most 0.007.
Values may be sent and summed in bfloat16 or wider, within the bound.
No kernel may reach another device: no remote copies, remote signals or barrier semaphores. Data moves between devices by JAX's collectives and lax.ppermute only.
A program may use at most 64 MiB of HBM per device.

```python
import jax
import jax.numpy as jnp
from jax import lax

SAMP = 4096
KWIN = 256
NTAB = 4
RANGE = 3
VOX = 2048
FRAMES = 128
DET_DEV = 1
DETS = 32
N_SLAB = 8
N_DET = 4


def draw_slab_range(key, part):
    lower_key, upper_key = jax.random.split(jax.random.fold_in(key, 11))
    detector_index = jnp.arange(DETS, dtype=jnp.int32)
    home = detector_index // (N_DET * DET_DEV)
    lower_reach = jax.random.randint(lower_key, (DETS,), 0, RANGE + 1)
    upper_reach = jax.random.randint(upper_key, (DETS,), 0, RANGE + 1)
    widest = detector_index % 7 == 0
    lower_reach = jnp.where(widest, RANGE, lower_reach)
    upper_reach = jnp.where(widest, RANGE, upper_reach)
    first_slab = jnp.maximum(home - lower_reach, 0)
    last_slab = jnp.minimum(home + upper_reach, N_SLAB - 1)
    return jnp.stack([first_slab, last_slab], axis=1).astype(jnp.int32)


def plant(entries, rng, smallest, largest):
    longest = entries.shape.index(max(entries.shape))
    spots = []
    for shift in (0, 1):
        where = [jax.random.randint(jax.random.fold_in(rng, axis), (), 0, length) for axis, length in enumerate(entries.shape)]
        where[longest] = (where[longest] + shift) % entries.shape[longest]
        spots.append(tuple(where))
    return entries.at[spots[0]].set(smallest).at[spots[1]].set(largest)


def block_levels(key, shape, cuts, smallest, top_value):
    def one(dim, parts):
        steps = jax.random.uniform(jax.random.fold_in(jax.random.fold_in(key, 6), dim), (parts,), jnp.float32, smallest / len(cuts), top_value / len(cuts))
        return jnp.repeat(jnp.exp(steps), shape[dim] // parts).reshape((-1,) + (1,) * (len(shape) - dim - 1))

    loudness = one(*cuts[0])
    for cut in cuts[1:]:
        loudness = loudness * one(*cut)
    return loudness


def normal_values(key, shape, deviation, bound, cuts=(), kind=jnp.bfloat16):
    array = jax.random.normal(key, shape, jnp.float32) * deviation
    if len(cuts) > 0:
        array = block_levels(key, shape, cuts, -0.22, 0.18) * array
    return jnp.clip(array, min=-bound, max=bound).astype(kind)


def setup_inputs(seed: int = 0) -> dict:
    splits = jax.random.split(jax.random.key(seed), 6)
    traces = normal_values(splits[0], (DETS, FRAMES, SAMP), 1.0, 6.0, ((0, 32),), jnp.float32)
    tables = normal_values(splits[1], (N_SLAB * NTAB, KWIN, N_SLAB * 0 + VOX), (4 * (2 * RANGE + 1) * DET_DEV * KWIN) ** -0.5, 0.0625, ((0, 8), (2, 4)))
    slab_range = draw_slab_range(jax.random.fold_in(splits[5], 71), 0)
    table_slot = plant(jax.random.randint(splits[3], (DETS, 2 * RANGE + 1), 0, NTAB), jax.random.fold_in(splits[3], 1), 0, NTAB - 1).astype(jnp.int32)
    sample_start = plant(jax.random.randint(splits[4], (DETS, 2 * RANGE + 1), 0, SAMP - KWIN + 1), jax.random.fold_in(splits[4], 1), 0, SAMP - KWIN).astype(jnp.int32)
    return {"traces": traces, "tables": tables, "slab_range": slab_range, "table_slot": table_slot, "sample_start": sample_start}


def windows_for(trace_rows, starts):
    def single(trace_row, first_index):
        return lax.dynamic_slice_in_dim(trace_row, first_index, KWIN, 1)
    return jax.vmap(single)(trace_rows, starts)


def reference(traces, tables, slab_range, table_slot, sample_start):
    group = N_DET * DET_DEV
    table_blocks = tables.reshape(N_SLAB, NTAB, KWIN, VOX)
    slot_values = jnp.arange(NTAB, dtype=jnp.int32)

    def one_slab(slab):
        stacked = jnp.zeros((N_DET, NTAB, FRAMES, KWIN), jnp.float32)
        for offset in range(-RANGE, RANGE + 1):
            home = slab - offset
            valid = (home >= 0) & (home < N_SLAB)
            clipped = jnp.clip(home, 0, N_SLAB - 1)
            first_row = (clipped * group).astype(jnp.int32)
            trace_rows = lax.dynamic_slice_in_dim(traces, first_row, group, 0).astype(jnp.bfloat16)
            ranges = lax.dynamic_slice_in_dim(slab_range, first_row, group, 0)
            slot_ids = lax.dynamic_slice_in_dim(table_slot, first_row, group, 0)[:, offset + RANGE]
            starts = lax.dynamic_slice_in_dim(sample_start, first_row, group, 0)[:, offset + RANGE]
            active = valid & (ranges[:, 0] <= slab) & (slab <= ranges[:, 1])
            windows = windows_for(trace_rows, starts).astype(jnp.float32)
            windows = windows.reshape(N_DET, DET_DEV, FRAMES, KWIN)
            onehot = ((slot_ids[:, None] == slot_values[None, :]) & active[:, None]).astype(jnp.float32)
            onehot = onehot.reshape(N_DET, DET_DEV, NTAB)
            stacked = stacked + jnp.einsum("kit,kifw->ktfw", onehot, windows)
        rounded = stacked.astype(jnp.bfloat16).astype(jnp.float32)
        weights = table_blocks[slab].astype(jnp.float32)
        return jnp.einsum("ktfw,twv->fv", rounded, weights)

    slabs = lax.map(one_slab, jnp.arange(N_SLAB, dtype=jnp.int32))
    return jnp.transpose(slabs, (1, 0, 2)).reshape(FRAMES, N_SLAB * VOX)
```

```python
import jax
import jax.numpy as jnp
from jax import lax
from jax.experimental import pallas as pl
from jax.experimental.pallas import tpu as pltpu
from jax.sharding import PartitionSpec as P

KWIN = 256
NTAB = 4
RANGE = 3
LANES = 128
CODE_ROWS = 8
OFFSETS = (0, 1, -1, 2, -2, 3, -3)


def rotated(x, axis, by):
    peers = lax.axis_size(axis)
    return lax.ppermute(x, axis, [(i, (i + by) % peers) for i in range(peers)])


def cut_kernel(place, starts, slots, ranges, traces, *rest):
    outs, held, sems = rest[: len(OFFSETS)], rest[-2], rest[-1]
    n_rows, width = held.shape[1], held.shape[2]
    last_base = traces.shape[2] - width
    copies, shifts = [], []
    for i, offset in enumerate(OFFSETS):
        start = starts[0, offset + RANGE]
        base = jnp.minimum(start // LANES * LANES, last_base)
        shifts.append(start - base)
        copies.append(
            pltpu.make_async_copy(
                traces.at[0, :, pl.ds(pl.multiple_of(base, LANES), width)], held.at[i], sems.at[i]
            )
        )
    for copy in copies:
        copy.start()
    for i, offset in enumerate(OFFSETS):
        target = place[0] + offset
        active = (
            (target >= 0) & (target < place[1]) & (ranges[0, 0] <= target) & (target <= ranges[0, 1])
        )
        code = jnp.where(active, slots[0, offset + RANGE], -1).astype(jnp.float32)
        outs[i][n_rows:, :] = jnp.full((CODE_ROWS, KWIN), code, jnp.float32).astype(jnp.bfloat16)
        copies[i].wait()
        back = jnp.where(shifts[i] == 0, 0, width - shifts[i])
        window = pltpu.roll(held[i], back, 1)[:, :KWIN]
        outs[i][:n_rows, :] = window.astype(jnp.bfloat16)


def bin_kernel(place, *refs):
    windows, outs = refs[: len(OFFSETS)], refs[len(OFFSETS):]
    peers = len(outs)
    rows = outs[0].shape[0]
    frames = rows * peers
    codes = [ref[frames : frames + 1, :].astype(jnp.float32) for ref in windows]
    for r in range(peers):
        first = pl.multiple_of((place[2] + r) % peers * rows, rows)
        parts = [ref[pl.ds(first, rows), :].astype(jnp.float32) for ref in windows]
        for t in range(NTAB):
            total = jnp.zeros((rows, KWIN), jnp.float32)
            for code, part in zip(codes, parts):
                total = total + jnp.where(code == t, part, 0.0)
            outs[r][:, t * KWIN : (t + 1) * KWIN] = total.astype(jnp.bfloat16)


def image_kernel(place, *refs):
    blocks, tables, out, stack = refs[:-3], refs[-3], refs[-2], refs[-1]
    peers = len(blocks)
    rows = blocks[0].shape[0]
    for r, block in enumerate(blocks):
        first = pl.multiple_of((place[2] + peers - r) % peers * rows, rows)
        stack[pl.ds(first, rows), :] = block[...]
    weights = tables[...].reshape(NTAB * KWIN, tables.shape[2])
    out[...] = jnp.dot(stack[...], weights, preferred_element_type=jnp.float32)


SMEM = pl.BlockSpec(memory_space=pltpu.SMEM)
VMEM = pl.BlockSpec(memory_space=pltpu.VMEM)
ANY = pl.BlockSpec(memory_space=pl.ANY)


def body(traces, tables, slab_range, table_slot, sample_start):
    peers = lax.axis_size("det")
    frames, voxels = traces.shape[1], tables.shape[2]
    rows = frames // peers
    place = jnp.stack(
        [lax.axis_index("slab"), jnp.int32(lax.axis_size("slab")), lax.axis_index("det")]
    ).astype(jnp.int32)
    n_off = len(OFFSETS)
    cut = pl.pallas_call(
        cut_kernel,
        in_specs=[SMEM, SMEM, SMEM, SMEM, ANY],
        out_specs=[VMEM] * n_off,
        out_shape=[jax.ShapeDtypeStruct((frames + CODE_ROWS, KWIN), jnp.bfloat16)] * n_off,
        scratch_shapes=[
            pltpu.VMEM((n_off, frames, KWIN + LANES), jnp.float32),
            pltpu.SemaphoreType.DMA((n_off,)),
        ],
        name="cut",
    )(place, sample_start, table_slot, slab_range, traces)
    arrived = [cut[0]] + [rotated(w, "slab", o) for w, o in zip(cut[1:], OFFSETS[1:])]
    pieces = pl.pallas_call(
        bin_kernel,
        in_specs=[SMEM] + [VMEM] * n_off,
        out_specs=[VMEM] * peers,
        out_shape=[jax.ShapeDtypeStruct((rows, NTAB * KWIN), jnp.bfloat16)] * peers,
        name="bin",
    )(place, *arrived)
    turns = sorted(range(1, peers), key=lambda r: (min(r, peers - r), r))
    shares = [pieces[0]] + [rotated(pieces[r], "det", r) for r in turns]
    total = shares[0].astype(jnp.float32)
    for share in shares[1:]:
        total = total + share.astype(jnp.float32)
    summed = total.astype(jnp.bfloat16)
    gathered = {r: rotated(summed, "det", r) for r in turns}
    blocks = [summed] + [gathered[r] for r in range(1, peers)]
    return pl.pallas_call(
        image_kernel,
        in_specs=[SMEM] + [VMEM] * (peers + 1),
        out_specs=VMEM,
        out_shape=jax.ShapeDtypeStruct((frames, voxels), jnp.float32),
        scratch_shapes=[pltpu.VMEM((frames, NTAB * KWIN), jnp.bfloat16)],
        name="image",
    )(place, *blocks, tables)


def solution(mesh):
    placed = (
        P(("slab", "det"), None, None),
        P("slab", None, "det"),
        P(("slab", "det"), None),
        P(("slab", "det"), None),
        P(("slab", "det"), None),
    )
    return jax.shard_map(
        body, mesh=mesh, in_specs=placed, out_specs=P(None, ("slab", "det")), check_vma=False
    )
```

```python
import jax
import jax.numpy as jnp
from jax import lax
from jax.experimental import pallas as pl
from jax.experimental.pallas import tpu as pltpu
from jax.sharding import PartitionSpec as P

KWIN = 256
NTAB = 4
RANGE = 3
LANES = 128
CODE_ROWS = 8
OFFSETS = (0, 1, -1, 2, -2, 3, -3)


def rotated(x, axis, by):
    peers = lax.axis_size(axis)
    return lax.ppermute(x, axis, [(i, (i + by) % peers) for i in range(peers)])


def near(x):
    return pltpu.with_memory_space_constraint(x, pltpu.VMEM)


def cut_kernel(starts, slots, ranges, traces, *rest):
    outs, held, sems = rest[: len(OFFSETS)], rest[-2], rest[-1]
    n_rows, width = held.shape[1], held.shape[2]
    last_base = traces.shape[2] - width
    copies, shifts = [], []
    for i, offset in enumerate(OFFSETS):
        start = starts[0, offset + RANGE]
        base = jnp.minimum(start // LANES * LANES, last_base)
        shifts.append(start - base)
        copies.append(
            pltpu.make_async_copy(
                traces.at[0, :, pl.ds(pl.multiple_of(base, LANES), width)], held.at[i], sems.at[i]
            )
        )
    for copy in copies:
        copy.start()
    for i, offset in enumerate(OFFSETS):
        target = lax.axis_index("slab") + offset
        active = (
            (target >= 0) & (target < lax.axis_size("slab")) & (ranges[0, 0] <= target) & (target <= ranges[0, 1])
        )
        code = jnp.where(active, slots[0, offset + RANGE], -1).astype(jnp.float32)
        outs[i][n_rows:, :] = jnp.full((CODE_ROWS, KWIN), code, jnp.float32).astype(jnp.bfloat16)
        copies[i].wait()
        back = jnp.where(shifts[i] == 0, 0, width - shifts[i])
        window = pltpu.roll(held[i], back, 1)[:, :KWIN]
        outs[i][:n_rows, :] = window.astype(jnp.bfloat16)


def bin_kernel(*refs):
    windows, outs = refs[: len(OFFSETS)], refs[len(OFFSETS):]
    peers = len(outs)
    rows = outs[0].shape[0]
    frames = rows * peers
    codes = [ref[frames : frames + 1, :].astype(jnp.float32) for ref in windows]
    for r in range(peers):
        first = pl.multiple_of((lax.axis_index("det") + r) % peers * rows, rows)
        parts = [ref[pl.ds(first, rows), :].astype(jnp.float32) for ref in windows]
        for t in range(NTAB):
            total = jnp.zeros((rows, KWIN), jnp.float32)
            for code, part in zip(codes, parts):
                total = total + jnp.where(code == t, part, 0.0)
            outs[r][:, t * KWIN : (t + 1) * KWIN] = total.astype(jnp.bfloat16)


def image_kernel(*refs):
    blocks, tables, out, stack = refs[:-3], refs[-3], refs[-2], refs[-1]
    peers = len(blocks)
    rows = blocks[0].shape[0]
    for r, block in enumerate(blocks):
        first = pl.multiple_of((lax.axis_index("det") + peers - r) % peers * rows, rows)
        stack[pl.ds(first, rows), :] = block[...]
    weights = tables[...].reshape(NTAB * KWIN, tables.shape[2])
    out[...] = jnp.dot(stack[...], weights, preferred_element_type=jnp.float32)


SMEM = pl.BlockSpec(memory_space=pltpu.SMEM)
VMEM = pl.BlockSpec(memory_space=pltpu.VMEM)
ANY = pl.BlockSpec(memory_space=pl.ANY)


def body(traces, tables, slab_range, table_slot, sample_start):
    peers = lax.axis_size("det")
    frames, voxels = traces.shape[1], tables.shape[2]
    rows = frames // peers
    n_off = len(OFFSETS)
    cut = pl.pallas_call(
        cut_kernel,
        in_specs=[SMEM, SMEM, SMEM, ANY],
        out_specs=[VMEM] * n_off,
        out_shape=[pltpu.VMEM((frames + CODE_ROWS, KWIN), jnp.bfloat16)] * n_off,
        scratch_shapes=[
            pltpu.VMEM((n_off, frames, KWIN + LANES), jnp.float32),
            pltpu.SemaphoreType.DMA((n_off,)),
        ],
        name="cut",
    )(sample_start, table_slot, slab_range, traces)
    arrived = [cut[0]] + [rotated(w, "slab", o) for w, o in zip(cut[1:], OFFSETS[1:])]
    pieces = pl.pallas_call(
        bin_kernel,
        in_specs=[VMEM] * n_off,
        out_specs=[VMEM] * peers,
        out_shape=[pltpu.VMEM((rows, NTAB * KWIN), jnp.bfloat16)] * peers,
        name="bin",
    )(*map(near, arrived))
    turns = sorted(range(1, peers), key=lambda r: (min(r, peers - r), r))
    shares = [pieces[0]] + [rotated(pieces[r], "det", r) for r in turns]
    total = shares[0].astype(jnp.float32)
    for share in shares[1:]:
        total = total + share.astype(jnp.float32)
    summed = total.astype(jnp.bfloat16)
    gathered = {r: rotated(summed, "det", r) for r in turns}
    blocks = [summed] + [gathered[r] for r in range(1, peers)]
    return pl.pallas_call(
        image_kernel,
        in_specs=[VMEM] * (peers + 1),
        out_specs=VMEM,
        out_shape=jax.ShapeDtypeStruct((frames, voxels), jnp.float32),
        scratch_shapes=[pltpu.VMEM((frames, NTAB * KWIN), jnp.bfloat16)],
        name="image",
    )(*map(near, blocks), near(tables))


def solution(mesh):
    placed = (
        P(("slab", "det"), None, None),
        P("slab", None, "det"),
        P(("slab", "det"), None),
        P(("slab", "det"), None),
        P(("slab", "det"), None),
    )
    return jax.shard_map(
        body, mesh=mesh, in_specs=placed, out_specs=P(None, ("slab", "det")), check_vma=False
    )
```

```python
import jax
import jax.numpy as jnp
from jax import lax
from jax.experimental import pallas as pl
from jax.experimental.pallas import tpu as pltpu
from jax.sharding import PartitionSpec as P

KWIN = 256
NTAB = 4
RANGE = 3
LANES = 128
CODE_ROWS = 8
OFFSETS = (0, 2, 3, -2, -3, 1, -1)


def rotated(x, axis, by):
    peers = lax.axis_size(axis)
    return lax.ppermute(x, axis, [(i, (i + by) % peers) for i in range(peers)])


def near(x):
    return pltpu.with_memory_space_constraint(x, pltpu.VMEM)


def cut_kernel(starts, slots, ranges, traces, *rest):
    outs, held, sems = rest[: len(OFFSETS)], rest[-2], rest[-1]
    n_rows, width = held.shape[1], held.shape[2]
    last_base = traces.shape[2] - width
    copies, shifts = [], []
    for i, offset in enumerate(OFFSETS):
        start = starts[0, offset + RANGE]
        base = jnp.minimum(start // LANES * LANES, last_base)
        shifts.append(start - base)
        copies.append(
            pltpu.make_async_copy(
                traces.at[0, :, pl.ds(pl.multiple_of(base, LANES), width)], held.at[i], sems.at[i]
            )
        )
    for copy in copies:
        copy.start()
    for i, offset in enumerate(OFFSETS):
        target = lax.axis_index("slab") + offset
        active = (
            (target >= 0) & (target < lax.axis_size("slab")) & (ranges[0, 0] <= target) & (target <= ranges[0, 1])
        )
        code = jnp.where(active, slots[0, offset + RANGE], -1).astype(jnp.float32)
        outs[i][n_rows:, :] = jnp.full((CODE_ROWS, KWIN), code, jnp.float32).astype(jnp.bfloat16)
        copies[i].wait()
        back = jnp.where(shifts[i] == 0, 0, width - shifts[i])
        window = pltpu.roll(held[i], back, 1)[:, :KWIN]
        outs[i][:n_rows, :] = window.astype(jnp.bfloat16)


def bin_kernel(*refs):
    windows, outs = refs[: len(OFFSETS)], refs[len(OFFSETS):]
    peers = len(outs)
    rows = outs[0].shape[0]
    frames = rows * peers
    codes = [ref[frames : frames + 1, :].astype(jnp.float32) for ref in windows]
    for r in range(peers):
        first = pl.multiple_of((lax.axis_index("det") + r) % peers * rows, rows)
        parts = [ref[pl.ds(first, rows), :].astype(jnp.float32) for ref in windows]
        for t in range(NTAB):
            total = jnp.zeros((rows, KWIN), jnp.float32)
            for code, part in zip(codes, parts):
                total = total + jnp.where(code == t, part, 0.0)
            outs[r][:, t * KWIN : (t + 1) * KWIN] = total.astype(jnp.bfloat16)


def image_kernel(*refs):
    blocks, tables, out, stack = refs[:-3], refs[-3], refs[-2], refs[-1]
    peers = len(blocks)
    rows = blocks[0].shape[0]
    for r, block in enumerate(blocks):
        first = pl.multiple_of((lax.axis_index("det") + peers - r) % peers * rows, rows)
        stack[pl.ds(first, rows), :] = block[...]
    weights = tables[...].reshape(NTAB * KWIN, tables.shape[2])
    out[...] = jnp.dot(stack[...], weights, preferred_element_type=jnp.float32)


SMEM = pl.BlockSpec(memory_space=pltpu.SMEM)
VMEM = pl.BlockSpec(memory_space=pltpu.VMEM)
ANY = pl.BlockSpec(memory_space=pl.ANY)


def body(traces, tables, slab_range, table_slot, sample_start):
    peers = lax.axis_size("det")
    frames, voxels = traces.shape[1], tables.shape[2]
    rows = frames // peers
    n_off = len(OFFSETS)
    cut = pl.pallas_call(
        cut_kernel,
        in_specs=[SMEM, SMEM, SMEM, ANY],
        out_specs=[VMEM] * n_off,
        out_shape=[pltpu.VMEM((frames + CODE_ROWS, KWIN), jnp.bfloat16)] * n_off,
        scratch_shapes=[
            pltpu.VMEM((n_off, frames, KWIN + LANES), jnp.float32),
            pltpu.SemaphoreType.DMA((n_off,)),
        ],
        name="cut",
    )(sample_start, table_slot, slab_range, traces)
    arrived = [cut[0]] + [rotated(w, "slab", o) for w, o in zip(cut[1:], OFFSETS[1:])]
    pieces = pl.pallas_call(
        bin_kernel,
        in_specs=[VMEM] * n_off,
        out_specs=[VMEM] * peers,
        out_shape=[pltpu.VMEM((rows, NTAB * KWIN), jnp.bfloat16)] * peers,
        name="bin",
    )(*map(near, arrived))
    turns = list(range(1, peers))
    shares = [pieces[0]] + [rotated(pieces[r], "det", r) for r in turns]
    total = shares[0].astype(jnp.float32)
    for share in shares[1:]:
        total = total + share.astype(jnp.float32)
    summed = total.astype(jnp.bfloat16)
    gathered = {r: rotated(summed, "det", r) for r in turns}
    blocks = [summed] + [gathered[r] for r in range(1, peers)]
    return pl.pallas_call(
        image_kernel,
        in_specs=[VMEM] * (peers + 1),
        out_specs=VMEM,
        out_shape=jax.ShapeDtypeStruct((frames, voxels), jnp.float32),
        scratch_shapes=[pltpu.VMEM((frames, NTAB * KWIN), jnp.bfloat16)],
        name="image",
    )(*map(near, blocks), near(tables))


def solution(mesh):
    placed = (
        P(("slab", "det"), None, None),
        P("slab", None, "det"),
        P(("slab", "det"), None),
        P(("slab", "det"), None),
        P(("slab", "det"), None),
    )
    return jax.shard_map(
        body, mesh=mesh, in_specs=placed, out_specs=P(None, ("slab", "det")), check_vma=False
    )
```
